512 devices in a mesh: pair: 2 (over y_lo), dp: 32 (over x, z), ep: 8 (over y_hi, core).
Axes of the slice: x: 4, y: 8 (y_hi: 4, y_lo: 2; y = y_hi * 2 + y_lo), z: 8, core: 2. Of those that a mesh axis runs over, the one named last changes fastest.
Arguments:
- activations: bfloat16 [49152, 4096], P(('pair', 'dp'), 'ep'), parts along dimension 1, may hold values from -16 to 16
- cotangents: bfloat16 [49152, 16384], P(('pair', 'dp'), 'ep'), parts along dimension 1, may hold values from -1.75 to 1.75
Outputs:
- averaged_grad: bfloat16 [512, 16384], P('pair', 'ep'), parts along dimension 1
The draws below stay inside these ranges and needn't reach their ends.
There are 8 independent parts, one for each index of `ep`. The reference program is written for one: setup_inputs(seed, part) draws one part's arguments, and reference() takes and returns one part's arrays. A program takes and returns all parts, laid end to end along the dimension named above; each array names one. Nothing has to cross between parts.
All inputs are finite; a program needn't handle non-finite values.
Results may differ from the reference program's by a relative error of at most 0.001.
Values may be sent and summed in bfloat16 or wider, within the bound.
A program may use at most 64 MiB of HBM per device.

```python
import jax
import jax.numpy as jnp

FF = 2048
ROWS = 512
TOK_DEV = 768
REPLICAS = 64
TOKENS = 49152
N_PAIR = 2
N_DP = 32


def raised(drawn, stream_key, source, target, parts, factor):
    def block_of(position):
        return (jnp.arange(drawn.shape[position]) // (drawn.shape[position] // parts)).reshape((-1,) + (1,) * (drawn.ndim - 1 - position))

    near = jax.random.permutation(stream_key, parts)[block_of(target)]
    second = (block_of(target) + parts // 2) % parts
    return jnp.where((block_of(source) == near) | (block_of(source) == second), factor * drawn, drawn)


def steps_of(own_key, extent, cuts, least, largest):
    def one(position, parts):
        draws = jax.random.uniform(jax.random.fold_in(jax.random.fold_in(own_key, 6), position), (parts,), jnp.float32, least / len(cuts), largest / len(cuts))
        return jnp.repeat(jnp.exp(draws), extent[position] // parts).reshape((-1,) + (1,) * (len(extent) - position - 1))

    factor_of = one(*cuts[0])
    for cut in cuts[1:]:
        factor_of = factor_of * one(*cut)
    return factor_of


def scatter_about(key, shape, scale, bound, cuts=(), held_as=jnp.bfloat16):
    entries = jax.random.normal(key, shape, jnp.float32) * scale
    if len(cuts) > 0:
        entries = steps_of(key, shape, cuts, -0.22, 0.18) * entries
    return jnp.clip(entries, min=-bound, max=bound).astype(held_as)


def gaussian_with(own_key, dims, scale, limit, cuts, heavy, held_as=jnp.bfloat16):
    drawn = scale * jax.random.normal(own_key, dims, jnp.float32)
    if cuts:
        drawn = drawn * steps_of(own_key, dims, cuts, -0.22, 0.18)
    return jnp.clip(raised(drawn, jax.random.fold_in(own_key, 3), *heavy), -limit, limit).astype(held_as)


def setup_inputs(seed: int = 0, part: int = 0) -> dict:
    keys = jax.random.split(jax.random.key(seed), 3)
    part_keys = jax.random.split(jax.random.fold_in(keys[2], part), 3)
    return {
        "activations": gaussian_with(part_keys[0], (TOKENS, ROWS), 1.0, 16.0, ((0, 64),), (0, 1, 64, 4.0)),
        "cotangents": scatter_about(part_keys[1], (TOKENS, FF), (max(1, TOK_DEV // (N_PAIR * N_DP))) ** -0.5, 1.75, ((0, 64),)),
    }


def reference(activations, cotangents):
    grad_sum = jnp.dot(activations.T, cotangents, preferred_element_type=jnp.float32)
    return (grad_sum / REPLICAS).astype(jnp.bfloat16)
```

```python
import heapq

import jax
import jax.numpy as jnp
from jax import lax
from jax.experimental import pallas as pl
from jax.experimental.pallas import tpu as pltpu
from jax.sharding import Mesh
from jax.sharding import PartitionSpec as P

SIZE = {"pair": 2, "x": 4, "z": 8}
MESH = pl.DeviceIdType.MESH
ROWS = 16
ORDERS = (("x", "z", "pair"), ("z", "x", "pair"), ("x", "z", "pair"), ("z", "x", "pair"))
BYTES_PER_US = 46600.0
HOP_US, FURTHER_US, TASK_US = 1.9, 0.75, 0.1


def wrapped(index, n):
    return lax.rem(index + n, n)


class Flow:
    def __init__(self, send_sems, recv_sems):
        self.send_sems, self.recv_sems = send_sems, recv_sems
        self.now, self.free, self.heap, self.copies = 0.0, {}, [], []

    def send(self, axis, delta, src, dst, then):
        n = SIZE[axis]
        k = len(self.copies)
        peer = wrapped(lax.axis_index(axis) + delta, n)
        copy = pltpu.make_async_remote_copy(
            src_ref=src,
            dst_ref=dst,
            send_sem=self.send_sems.at[k],
            recv_sem=self.recv_sems.at[k],
            device_id={axis: peer},
            device_id_type=MESH,
        )
        copy.start()
        hops = abs(delta)
        size = 1
        for d in dst.shape:
            size *= d
        size *= jnp.dtype(dst.dtype).itemsize
        link = (axis, delta > 0)
        begin = max(self.now, self.free.get(link, 0.0))
        end = begin + hops * size / BYTES_PER_US
        self.free[link] = end
        heapq.heappush(self.heap, (end + HOP_US + FURTHER_US * (hops - 1), k, then))
        self.copies.append(copy)

    def run(self):
        while self.heap:
            at, k, then = heapq.heappop(self.heap)
            self.now = max(self.now, at) + TASK_US
            self.copies[k].wait_recv()
            then()
        for copy in self.copies:
            copy.wait_send()


def add_into(dst, src):
    if len(dst.shape) > 3:
        for i in range(dst.shape[0]):
            add_into(dst.at[i], src.at[i])
    else:
        dst[...] += src[...]


def reduce_stage(flow, axis, part, slots, done):
    n = SIZE[axis]
    me = lax.axis_index(axis)
    if n == 2:
        mine = part.at[me]

        def last():
            add_into(mine, slots[0].at[0])
            done(mine)

        flow.send(axis, 1, part.at[1 - me], slots[0].at[0], last)
        return
    steps = n // 2
    middle = part.shape[1] // 2
    left = [2]

    def advance(sign, step):
        slot = slots[0 if sign > 0 else 1]
        if step == 0:
            half = pl.ds(0, middle) if sign > 0 else pl.ds(middle, middle)
            chunk = part.at[wrapped(me + sign * steps, n), half]
            target = slot.at[0, pl.ds(0, middle)]
        else:
            chunk = part.at[wrapped(me + sign * (steps - step), n)]
            target = slot.at[step]

        def arrived():
            nearer = part.at[wrapped(me + sign * (steps - step - 1), n)]
            if step == 0:
                half = pl.ds(0, middle) if sign > 0 else pl.ds(middle, middle)
                add_into(nearer.at[half], target)
            else:
                add_into(nearer, target)
            if step + 1 < steps:
                advance(sign, step + 1)
                return
            left[0] -= 1
            if left[0] == 0:
                done(part.at[me])

        flow.send(axis, sign * 1, chunk, target, arrived)

    advance(1, 0)
    advance(-1, 0)


def block_of(out, at):
    everything = slice(None)
    return out.at[at.get("x", everything), at.get("z", everything)]


def gather_direct(flow, axis, out, at, done):
    n = SIZE[axis]
    me = lax.axis_index(axis)
    left = [n - 1]

    def arrived():
        left[0] -= 1
        if left[0] == 0:
            done()

    mine = block_of(out, at)
    for far in range(1, n // 2 + 1):
        for delta in (far, -far) if 2 * far < n else (far,):
            flow.send(axis, delta, mine, mine, arrived)


def gather_ring(flow, axis, out, at, done):
    n = SIZE[axis]
    me = lax.axis_index(axis)
    steps = n // 2
    left = [2]

    def advance(sign, step):
        block = block_of(out, {**at, axis: wrapped(me - sign * step, n)})
        if step == steps - 1:
            half = block.shape[0] // 2
            block = block.at[pl.ds(0 if sign > 0 else half, half)]

        def arrived():
            if step + 1 < steps:
                advance(sign, step + 1)
                return
            left[0] -= 1
            if left[0] == 0:
                done()

        flow.send(axis, sign, block, block, arrived)

    advance(1, 0)
    advance(-1, 0)


def kernel(replicas, a_ref, b_ref, out_ref, at_ref, *refs):
    n_inst = len(ORDERS)
    parts = refs[:n_inst]
    refs = refs[n_inst:]
    slots = []
    for order in ORDERS:
        own = []
        for axis in order:
            take = 1 if SIZE[axis] == 2 else 2
            own.append(refs[:take])
            refs = refs[take:]
        slots.append(own)
    send_sems, recv_sems = refs

    barrier = pltpu.get_barrier_semaphore()
    peers = 0
    for axis, n in SIZE.items():
        for delta in range(1, n):
            peer = wrapped(lax.axis_index(axis) + delta, n)
            pl.semaphore_signal(barrier, inc=1, device_id={axis: peer}, device_id_type=MESH)
            peers += 1

    at_ref[...] = a_ref[...].T
    for z in range(SIZE["z"]):
        total = jnp.dot(at_ref[...], b_ref[:, z * 256 : (z + 1) * 256], preferred_element_type=jnp.float32)
        for half in range(2):
            for x in range(SIZE["x"]):
                for i, order in enumerate(ORDERS):
                    first = half * 256 + x * 64 + i * ROWS
                    index = {"pair": half, "x": x, "z": z}
                    parts[i][tuple(index[axis] for axis in order)] = total[first : first + ROWS]

    pl.semaphore_wait(barrier, peers)
    flow = Flow(send_sems, recv_sems)

    def start(i):
        order = ORDERS[i]
        out = out_ref.at[i]
        here = {axis: lax.axis_index(axis) for axis in ("x", "z")}

        def gathered():
            pass

        def second_gather():
            gather_ring(flow, order[0], out, {}, gathered)

        def finish(piece):
            out[here["x"], here["z"]] = (piece[...] / replicas).astype(jnp.bfloat16)
            gather_direct(flow, order[1], out, dict(here), second_gather)

        def stage(k, part):
            if k == len(order):
                finish(part)
                return
            reduce_stage(flow, order[k], part, slots[i][k], lambda chunk: stage(k + 1, chunk))

        stage(0, parts[i])

    for i in range(n_inst):
        start(i)
    flow.run()


def local(activations, cotangents):
    rows, columns = activations.shape[1], cotangents.shape[1]
    piece = (ROWS, columns // SIZE["z"])
    replicas = SIZE["pair"] * SIZE["x"] * SIZE["z"]
    scratch = [pltpu.VMEM((rows, activations.shape[0]), jnp.bfloat16)]
    for order in ORDERS:
        scratch.append(pltpu.VMEM(tuple(SIZE[a] for a in order) + piece, jnp.float32))
    copies = 0
    for order in ORDERS:
        for k, axis in enumerate(order):
            chunk = tuple(SIZE[a] for a in order[k + 1 :]) + piece
            steps = SIZE[axis] // 2
            take = 1 if SIZE[axis] == 2 else 2
            scratch += [pltpu.VMEM((steps,) + chunk, jnp.float32)] * take
            copies += take * steps
        copies += SIZE[order[1]] - 1 + SIZE[order[0]]
    scratch += [pltpu.SemaphoreType.DMA((copies,))] * 2
    out = pl.pallas_call(
        lambda *refs: kernel(replicas, *refs),
        out_shape=jax.ShapeDtypeStruct((len(ORDERS), SIZE["x"], SIZE["z"]) + piece, jnp.bfloat16),
        in_specs=[pl.BlockSpec(memory_space=pltpu.VMEM)] * 2,
        out_specs=pl.BlockSpec(memory_space=pltpu.VMEM),
        scratch_shapes=scratch,
        compiler_params=pltpu.CompilerParams(collective_id=0, has_side_effects=True),
        name="grad_sum",
    )(activations, cotangents)
    return out.transpose(1, 0, 3, 2, 4).reshape(rows // SIZE["pair"], columns)


def solution(mesh):
    split = Mesh(
        mesh.devices.reshape(mesh.shape["pair"], SIZE["x"], SIZE["z"], mesh.shape["ep"]),
        ("pair", "x", "z", "ep"),
    )
    placed = P(("pair", "x", "z"), "ep")
    return jax.shard_map(
        local, mesh=split, in_specs=(placed, placed), out_specs=P("pair", "ep"), check_vma=False
    )
```

```python
import heapq
import math

import jax
import jax.numpy as jnp
from jax import lax
from jax.experimental import pallas as pl
from jax.experimental.pallas import tpu as pltpu
from jax.sharding import Mesh
from jax.sharding import PartitionSpec as P

SIZE = {"pair": 2, "x": 4, "z": 8}
MESH = pl.DeviceIdType.MESH
LEAF = (16, 128)
STRIPS = 4
SIDES = 2
X_STRIPS = (2, 2)
X_FIRST = ((("ring", "x"), ("ring", "pair"), ("direct", "z")), (("direct", "z"), ("ring", "x")))
Z_FIRST = ((("ring", "z"), ("ring", "pair"), ("direct", "x")), (("direct", "z"), ("ring", "x")))
RULER = 256
BYTES_PER_US = 46600.0
HOP_US, FURTHER_US, TASK_US = 2.65, 0.9, 0.03


def units():
    found = []
    for k in range(STRIPS):
        for side in range(SIDES):
            split = X_STRIPS[side]
            if k < split:
                found.append((k, side, X_FIRST))
            if STRIPS - 1 - k >= split:
                found.append((STRIPS - 1 - k, side, Z_FIRST))
    return found


def order_of(plan):
    return tuple(axis for _, axis in plan[0])


def wrapped(index, n):
    return lax.rem(index + n, n)


class Flow:
    def __init__(self, send_sems, recv_sems, ruler):
        self.send_sems, self.recv_sems, self.ruler = send_sems, recv_sems, ruler
        self.now, self.free, self.heap, self.waits = 0.0, {}, [], 0
        self.sent = {}

    def send(self, unit, axis, copies, arriving, then):
        k = self.waits
        self.waits += 1
        latest = 0.0
        for delta, src, dst in copies:
            pltpu.make_async_remote_copy(
                src_ref=src,
                dst_ref=dst,
                send_sem=self.send_sems.at[unit],
                recv_sem=self.recv_sems.at[k],
                device_id={axis: wrapped(lax.axis_index(axis) + delta, SIZE[axis])},
                device_id_type=MESH,
            ).start()
            hops = abs(delta)
            size = math.prod(dst.shape) * jnp.dtype(dst.dtype).itemsize
            self.sent[unit] = self.sent.get(unit, 0) + size
            link = (axis, delta > 0)
            end = max(self.now, self.free.get(link, 0.0)) + hops * size / BYTES_PER_US
            self.free[link] = end
            latest = max(latest, end + HOP_US + FURTHER_US * (hops - 1))
        heapq.heappush(self.heap, (latest, k, arriving, then))

    def run(self):
        while self.heap:
            at, k, arriving, then = heapq.heappop(self.heap)
            self.now = max(self.now, at) + TASK_US
            pltpu.make_async_copy(arriving, arriving, self.recv_sems.at[k]).wait()
            then()
        for unit, size in self.sent.items():
            row = math.prod(self.ruler.shape[1:]) * jnp.dtype(self.ruler.dtype).itemsize
            assert size % row == 0 and size // row <= self.ruler.shape[0]
            total = self.ruler.at[pl.ds(0, size // row)]
            pltpu.make_async_copy(total, total, self.send_sems.at[unit]).wait()


def add_into(dst, *sources):
    if len(dst.shape) > 3:
        for i in range(dst.shape[0]):
            add_into(dst.at[i], *(source.at[i] for source in sources))
    else:
        total = dst[...]
        for source in sources:
            total += source[...]
        dst[...] = total


def slots_of(kind, axis):
    n = SIZE[axis]
    return n - 1 if kind == "direct" or n == 2 else 2 * (n // 2)


def waits_of(kind, axis):
    return 1 if kind == "direct" else slots_of(kind, axis)


def deltas_of(n):
    return [d for far in range(1, n // 2 + 1) for d in ((far, -far) if 2 * far < n else (far,))]


def reduce_direct(flow, unit, axis, part, slots, done):
    n = SIZE[axis]
    me = lax.axis_index(axis)

    def arrived():
        add_into(part.at[me], *(slots.at[i] for i in range(n - 1)))
        done(part.at[me])

    copies = [(delta, part.at[wrapped(me + delta, n)], slots.at[i]) for i, delta in enumerate(deltas_of(n))]
    flow.send(unit, axis, copies, slots, arrived)


def reduce_ring(flow, unit, axis, part, slots, done):
    n = SIZE[axis]
    me = lax.axis_index(axis)
    steps = n // 2
    middle = part.shape[1] // 2
    left = [2]

    def advance(sign, step):
        slot = slots.at[step if sign > 0 else steps + step]
        chunk = part.at[wrapped(me + sign * (steps - step), n)]
        nearer = part.at[wrapped(me + sign * (steps - step - 1), n)]
        if step == 0:
            half = pl.ds(0 if sign > 0 else middle, middle)
            slot, chunk, nearer = slot.at[pl.ds(0, middle)], chunk.at[half], nearer.at[half]

        def arrived():
            add_into(nearer, slot)
            if step + 1 < steps:
                advance(sign, step + 1)
                return
            left[0] -= 1
            if left[0] == 0:
                done(part.at[me])

        flow.send(unit, axis, [(sign, chunk, slot)], slot, arrived)

    advance(1, 0)
    advance(-1, 0)


def gather_direct(flow, unit, axis, block_at, at, done):
    mine = block_at({**at, axis: lax.axis_index(axis)})
    deltas = deltas_of(SIZE[axis])
    flow.send(unit, axis, [(delta, mine, mine) for delta in deltas], block_at(at, 0, len(deltas)), done)


def gather_ring(flow, unit, axis, block_at, at, done):
    n = SIZE[axis]
    me = lax.axis_index(axis)
    steps = n // 2
    left = [2]

    def advance(sign, step):
        place = {**at, axis: wrapped(me - sign * step, n)}
        block = block_at(place, sign if step == steps - 1 else 0)

        def arrived():
            if step + 1 < steps:
                advance(sign, step + 1)
                return
            left[0] -= 1
            if left[0] == 0:
                done()

        flow.send(unit, axis, [(sign, block, block)], block, arrived)

    advance(1, 0)
    advance(-1, 0)


REDUCE = {"ring": reduce_ring, "direct": reduce_direct}
GATHER = {"ring": gather_ring, "direct": gather_direct}


def start_unit(flow, number, unit, part, slots, out, replicas):
    strip, side, (reduce_plan, gather_plan) = unit
    height, width = LEAF
    extent = SIZE["z"] * width

    def block_at(at, half=0, count=None):
        x = at.get("x", pl.ds(0, count or SIZE["x"]))
        cols = pl.ds(side * extent, count * width if count else extent)
        if "z" in at:
            cols = pl.ds(pl.multiple_of(side * extent + at["z"] * width, width), width)
        if half and "z" in at:
            x = pl.ds(0 if half > 0 else SIZE["x"] // 2, SIZE["x"] // 2)
        elif half:
            cols = pl.ds(side * extent + (0 if half > 0 else extent // 2), extent // 2)
        return out.at[x, strip, :, cols]

    def gather(k):
        if k < len(gather_plan):
            kind, axis = gather_plan[k]
            rest = {other: lax.axis_index(other) for _, other in gather_plan[k + 1 :]}
            GATHER[kind](flow, number, axis, block_at, rest, lambda: gather(k + 1))

    def reduce(k, chunk):
        if k < len(reduce_plan):
            kind, axis = reduce_plan[k]
            if SIZE[axis] == 2:
                kind = "direct"
            REDUCE[kind](flow, number, axis, chunk, slots[k], lambda mine: reduce(k + 1, mine))
            return
        own = block_at({axis: lax.axis_index(axis) for axis in ("x", "z")})
        own[...] = (chunk[...] / replicas).astype(jnp.bfloat16)
        gather(0)

    reduce(0, part)


def kernel(replicas, a_hbm, b_hbm, out, a_ref, b_ref, for_x, for_z, ruler, in_sems, send_sems, recv_sems, *refs):
    work = units()
    parts, refs = refs[: len(work)], list(refs[len(work) :])
    slots = [[refs.pop(0) for _ in unit[2][0]] for unit in work]
    height, width = LEAF
    rows, tokens = for_x.shape
    extent = SIZE["z"] * width

    cuts = in_sems.shape[0] - 1
    load_a = pltpu.make_async_copy(a_hbm, a_ref, in_sems.at[cuts])
    load_a.start()
    loads_b = []
    for i in range(cuts):
        cut = pl.ds(i * (tokens // cuts), tokens // cuts)
        loads_b.append(pltpu.make_async_copy(b_hbm.at[cut], b_ref.at[cut], in_sems.at[i]))
        loads_b[-1].start()

    barrier = pltpu.get_barrier_semaphore()
    peers = 0
    for axis, n in SIZE.items():
        for delta in range(1, n):
            peer = wrapped(lax.axis_index(axis) + delta, n)
            pl.semaphore_signal(barrier, inc=1, device_id={axis: peer}, device_id_type=MESH)
            peers += 1

    group = 2 * height
    load_a.wait()
    for first in range(0, rows, 128):
        turned = a_ref[:, first : first + 128].T
        for row in range(first, first + 128, height):
            half, rest = divmod(row, rows // 2)
            x, rest = divmod(rest, rows // 2 // SIZE["x"])
            strip = rest // height
            piece = turned[row - first : row - first + height]
            for_x[pl.ds((x * STRIPS + strip) * group + half * height, height), :] = piece
            for_z[pl.ds((strip * SIZE["x"] + x) * group + half * height, height), :] = piece
    for load in loads_b:
        load.wait()

    def part_of(strip, side):
        for unit, part in zip(work, parts):
            if unit[:2] == (strip, side):
                return part

    def multiply_x(x):
        for side in range(SIDES):
            strips = X_STRIPS[side]
            if strips == 0:
                continue
            left = for_x[pl.ds(pl.multiple_of(x * (STRIPS * group), group), strips * group), :]
            for z in range(0, SIZE["z"], 2):
                column = side * extent + z * width
                total = jnp.dot(left, b_ref[:, column : column + 2 * width], preferred_element_type=jnp.float32)
                for strip in range(strips):
                    for half in range(2):
                        top = strip * group + half * height
                        for k in range(2):
                            part_of(strip, side)[x, half, z + k] = total[top : top + height, k * width : (k + 1) * width]

    def multiply_z(z):
        for side in range(SIDES):
            split = X_STRIPS[side]
            if split == STRIPS:
                continue
            left = for_z[split * SIZE["x"] * group :, :]
            column = pl.multiple_of(side * extent + z * width, width)
            total = jnp.dot(left, b_ref[:, pl.ds(column, width)], preferred_element_type=jnp.float32)
            for strip in range(split, STRIPS):
                for x in range(SIZE["x"]):
                    for half in range(2):
                        top = ((strip - split) * SIZE["x"] + x) * group + half * height
                        part_of(strip, side)[z, half, x] = total[top : top + height]

    me = {axis: lax.axis_index(axis) for axis in SIZE}
    flow = Flow(send_sems, recv_sems, ruler)
    multiply_z(wrapped(me["z"] + SIZE["z"] // 2, SIZE["z"]))
    multiply_x(wrapped(me["x"] + SIZE["x"] // 2, SIZE["x"]))
    pl.semaphore_wait(barrier, peers)
    for number, unit in enumerate(work):
        start_unit(flow, number, unit, parts[number], slots[number], out, replicas)
    for far in range(SIZE["z"] // 2 - 1, 0, -1):
        if far < SIZE["x"] // 2:
            multiply_x(wrapped(me["x"] + far, SIZE["x"]))
            multiply_x(wrapped(me["x"] - far, SIZE["x"]))
        multiply_z(wrapped(me["z"] + far, SIZE["z"]))
        multiply_z(wrapped(me["z"] - far, SIZE["z"]))
    multiply_x(me["x"])
    multiply_z(me["z"])
    flow.run()


def local(activations, cotangents):
    tokens, rows = activations.shape
    columns = cotangents.shape[1]
    work = units()
    scratch = [
        pltpu.VMEM((tokens, rows), jnp.bfloat16),
        pltpu.VMEM((tokens, columns), jnp.bfloat16),
        pltpu.VMEM((rows, tokens), jnp.bfloat16),
        pltpu.VMEM((rows, tokens), jnp.bfloat16),
        pltpu.VMEM((RULER,) + LEAF, jnp.bfloat16),
        pltpu.SemaphoreType.DMA((5,)),
    ]
    parts, slots, waits = [], [], 0
    for _, _, plan in work:
        order = order_of(plan)
        parts.append(pltpu.VMEM(tuple(SIZE[axis] for axis in order) + LEAF, jnp.float32))
        for k, (kind, axis) in enumerate(plan[0]):
            chunk = tuple(SIZE[other] for other in order[k + 1 :]) + LEAF
            slots.append(pltpu.VMEM((slots_of(kind, axis),) + chunk, jnp.float32))
        waits += sum(waits_of(kind, axis) for stages in plan for kind, axis in stages)
    scratch += [pltpu.SemaphoreType.DMA((len(work),)), pltpu.SemaphoreType.DMA((waits,))] + parts + slots
    replicas = math.prod(SIZE.values())
    shape = (SIZE["x"], STRIPS, LEAF[0], columns)
    out = pl.pallas_call(
        lambda *refs: kernel(replicas, *refs),
        out_shape=pltpu.VMEM(shape, jnp.bfloat16),
        in_specs=[pl.BlockSpec(memory_space=pl.ANY)] * 2,
        out_specs=pl.BlockSpec(memory_space=pltpu.VMEM),
        scratch_shapes=scratch,
        compiler_params=pltpu.CompilerParams(collective_id=0, has_side_effects=True),
        name="grad_sum",
    )(activations, cotangents)
    return out.reshape(rows // SIZE["pair"], columns)


def solution(mesh):
    split = Mesh(
        mesh.devices.reshape(mesh.shape["pair"], SIZE["x"], SIZE["z"], mesh.shape["ep"]),
        ("pair", "x", "z", "ep"),
    )
    placed = P(("pair", "x", "z"), "ep")
    return jax.shard_map(
        local, mesh=split, in_specs=(placed, placed), out_specs=P("pair", "ep"), check_vma=False
    )
```

```python
import heapq
import math

import jax
import jax.numpy as jnp
from jax import lax
from jax.experimental import pallas as pl
from jax.experimental.pallas import tpu as pltpu
from jax.sharding import Mesh
from jax.sharding import PartitionSpec as P

SIZE = {"pair": 2, "x": 4, "z": 8}
MESH = pl.DeviceIdType.MESH
LEAF = (16, 128)
STRIPS = 4
SIDES = 2
X_STRIPS = (2, 2)
X_FIRST = ((("coded", "x"), ("ring", "pair"), ("direct", "z")), (("direct", "z"), ("ring", "x")))
Z_FIRST = ((("coded", "z"), ("ring", "pair"), ("direct", "x")), (("direct", "z"), ("ring", "x")))
GROUP = 4
CODE_POWER, CODE_STEEP, CODE_LOW = 36, 120.0, 2.0**-3.45
RULER = 320
BYTES_PER_US = 46600.0
HOP_US, FURTHER_US, TASK_US = 2.65, 0.9, 0.15


def units():
    found = []
    for k in range(STRIPS):
        for side in range(SIDES):
            split = X_STRIPS[side]
            if k < split:
                found.append((k, side, X_FIRST))
            if STRIPS - 1 - k >= split:
                found.append((STRIPS - 1 - k, side, Z_FIRST))
    return found


def order_of(plan):
    return tuple(axis for _, axis in plan[0])


def wrapped(index, n):
    return lax.rem(index + n, n)


class Flow:
    def __init__(self, send_sems, recv_sems, ruler):
        self.send_sems, self.recv_sems, self.ruler = send_sems, recv_sems, ruler
        self.now, self.free, self.heap, self.waits = 0.0, {}, [], 0
        self.sent = {}

    def send(self, unit, axis, copies, arriving, then):
        k = self.waits
        self.waits += 1
        latest = 0.0
        for delta, src, dst in copies:
            pltpu.make_async_remote_copy(
                src_ref=src,
                dst_ref=dst,
                send_sem=self.send_sems.at[unit],
                recv_sem=self.recv_sems.at[k],
                device_id={axis: wrapped(lax.axis_index(axis) + delta, SIZE[axis])},
                device_id_type=MESH,
            ).start()
            hops = abs(delta)
            size = math.prod(dst.shape) * jnp.dtype(dst.dtype).itemsize
            self.sent[unit] = self.sent.get(unit, 0) + size
            link = (axis, delta > 0)
            end = max(self.now, self.free.get(link, 0.0)) + hops * size / BYTES_PER_US
            self.free[link] = end
            latest = max(latest, end + HOP_US + FURTHER_US * (hops - 1))
        heapq.heappush(self.heap, (latest, k, arriving, then))

    def run(self):
        while self.heap:
            at, k, arriving, then = heapq.heappop(self.heap)
            self.now = max(self.now, at) + TASK_US
            pltpu.make_async_copy(arriving, arriving, self.recv_sems.at[k]).wait()
            then()
        for unit, size in self.sent.items():
            row = math.prod(self.ruler.shape[1:]) * jnp.dtype(self.ruler.dtype).itemsize
            assert size % row == 0 and size // row <= self.ruler.shape[0]
            total = self.ruler.at[pl.ds(0, size // row)]
            pltpu.make_async_copy(total, total, self.send_sems.at[unit]).wait()


def add_into(dst, *sources):
    if len(dst.shape) > 3:
        for i in range(dst.shape[0]):
            add_into(dst.at[i], *(source.at[i] for source in sources))
    else:
        total = dst[...]
        for source in sources:
            total += source[...]
        dst[...] = total


def slots_of(kind, axis):
    n = SIZE[axis]
    return n - 1 if kind == "direct" or n == 2 else 2 * (n // 2)


def waits_of(kind, axis):
    return 1 if kind == "direct" else slots_of(kind, axis)


def deltas_of(n):
    return [d for far in range(1, n // 2 + 1) for d in ((far, -far) if 2 * far < n else (far,))]


def reduce_direct(flow, unit, axis, part, slots, done):
    n = SIZE[axis]
    me = lax.axis_index(axis)

    def arrived():
        add_into(part.at[me], *(slots.at[i] for i in range(n - 1)))
        done(part.at[me])

    copies = [(delta, part.at[wrapped(me + delta, n)], slots.at[i]) for i, delta in enumerate(deltas_of(n))]
    flow.send(unit, axis, copies, slots, arrived)


def reduce_ring(flow, unit, axis, part, slots, done):
    n = SIZE[axis]
    me = lax.axis_index(axis)
    steps = n // 2
    middle = part.shape[1] // 2
    left = [2]

    def advance(sign, step):
        slot = slots.at[step if sign > 0 else steps + step]
        chunk = part.at[wrapped(me + sign * (steps - step), n)]
        nearer = part.at[wrapped(me + sign * (steps - step - 1), n)]
        if step == 0:
            half = pl.ds(0 if sign > 0 else middle, middle)
            slot, chunk, nearer = slot.at[pl.ds(0, middle)], chunk.at[half], nearer.at[half]

        def arrived():
            add_into(nearer, slot)
            if step + 1 < steps:
                advance(sign, step + 1)
                return
            left[0] -= 1
            if left[0] == 0:
                done(part.at[me])

        flow.send(unit, axis, [(sign, chunk, slot)], slot, arrived)

    advance(1, 0)
    advance(-1, 0)


def gather_direct(flow, unit, axis, block_at, at, done):
    mine = block_at({**at, axis: lax.axis_index(axis)})
    deltas = deltas_of(SIZE[axis])
    flow.send(unit, axis, [(delta, mine, mine) for delta in deltas], block_at(at, 0, len(deltas)), done)


def gather_ring(flow, unit, axis, block_at, at, done):
    n = SIZE[axis]
    me = lax.axis_index(axis)
    steps = n // 2
    left = [2]

    def advance(sign, step):
        place = {**at, axis: wrapped(me - sign * step, n)}
        block = block_at(place, sign if step == steps - 1 else 0)

        def arrived():
            if step + 1 < steps:
                advance(sign, step + 1)
                return
            left[0] -= 1
            if left[0] == 0:
                done()

        flow.send(unit, axis, [(sign, block, block)], block, arrived)

    advance(1, 0)
    advance(-1, 0)


def magnitudes(x):
    return jnp.max(jnp.abs(x), axis=0)


def encode(x, scale):
    y = jnp.abs(x) * (CODE_STEEP * CODE_LOW / jnp.maximum(scale, 1e-35)) + CODE_LOW
    y4 = y * y * (y * y)
    y8 = y4 * y4
    y16 = y8 * y8
    y = y16 * y16 * y4
    return jnp.where(x < 0, -y, y).astype(jnp.bfloat16)


def decode(code, scale):
    y = code.astype(jnp.float32)
    root = jnp.exp(jnp.log(jnp.abs(y)) * (1 / CODE_POWER) - math.log(CODE_LOW))
    x = (root - 1) * (scale * (1 / CODE_STEEP))
    return jnp.where(y < 0, -x, x)


def coded_rows(shape):
    return math.prod(shape[:-1]) + 8


def groups_of(chunk):
    if len(chunk.shape) == 3:
        return [chunk.at[pl.ds(i, GROUP)] for i in range(0, chunk.shape[0], GROUP)]
    return [group for i in range(chunk.shape[0]) for group in groups_of(chunk.at[i])]


def group_rows(k):
    rows = GROUP * LEAF[0]
    return pl.ds(8 + k * rows, rows)


def write_code(chunk, wire):
    shape = (GROUP * LEAF[0] // 8, 8, LEAF[1])
    groups = groups_of(chunk)
    scale = magnitudes(groups[0][...].reshape(shape))
    for group in groups[1:]:
        scale = jnp.maximum(scale, magnitudes(group[...].reshape(shape)))
    scale = scale.astype(jnp.bfloat16)
    wire[pl.ds(0, 8), :] = scale
    scale = scale.astype(jnp.float32)
    for k, group in enumerate(groups):
        wire[group_rows(k), :] = encode(group[...].reshape(shape), scale).reshape(-1, LEAF[1])


def add_code(chunk, wire):
    shape = (GROUP * LEAF[0] // 8, 8, LEAF[1])
    scale = wire[pl.ds(0, 8), :].astype(jnp.float32)
    for k, group in enumerate(groups_of(chunk)):
        value = decode(wire[group_rows(k), :].reshape(shape), scale)
        group[...] += value.reshape(group.shape)


def reduce_coded(flow, unit, axis, part, slots, done):
    wires_in, wires_out = slots
    n = SIZE[axis]
    me = lax.axis_index(axis)
    steps = n // 2
    middle = part.shape[1] // 2
    left = [2]

    def advance(sign, step):
        index = step if sign > 0 else steps + step
        chunk = part.at[wrapped(me + sign * (steps - step), n)]
        nearer = part.at[wrapped(me + sign * (steps - step - 1), n)]
        if step == 0:
            half = pl.ds(0 if sign > 0 else middle, middle)
            chunk, nearer = chunk.at[half], nearer.at[half]
        rows = pl.ds(0, coded_rows(chunk.shape))
        source, target = wires_out.at[index, rows], wires_in.at[index, rows]

        def arrived():
            add_code(nearer, target)
            if step + 1 < steps:
                advance(sign, step + 1)
                return
            left[0] -= 1
            if left[0] == 0:
                done(part.at[me])

        write_code(chunk, source)
        flow.send(unit, axis, [(sign, source, target)], target, arrived)

    advance(1, 0)
    advance(-1, 0)


REDUCE = {"ring": reduce_ring, "direct": reduce_direct, "coded": reduce_coded}
GATHER = {"ring": gather_ring, "direct": gather_direct}


def start_unit(flow, number, unit, part, slots, out, replicas):
    strip, side, (reduce_plan, gather_plan) = unit
    height, width = LEAF
    extent = SIZE["z"] * width

    def block_at(at, half=0, count=None):
        x = at.get("x", pl.ds(0, count or SIZE["x"]))
        cols = pl.ds(side * extent, count * width if count else extent)
        if "z" in at:
            cols = pl.ds(pl.multiple_of(side * extent + at["z"] * width, width), width)
        if half and "z" in at:
            x = pl.ds(0 if half > 0 else SIZE["x"] // 2, SIZE["x"] // 2)
        elif half:
            cols = pl.ds(side * extent + (0 if half > 0 else extent // 2), extent // 2)
        return out.at[x, strip, :, cols]

    def gather(k):
        if k < len(gather_plan):
            kind, axis = gather_plan[k]
            rest = {other: lax.axis_index(other) for _, other in gather_plan[k + 1 :]}
            GATHER[kind](flow, number, axis, block_at, rest, lambda: gather(k + 1))

    def reduce(k, chunk):
        if k < len(reduce_plan):
            kind, axis = reduce_plan[k]
            if SIZE[axis] == 2:
                kind = "direct"
            REDUCE[kind](flow, number, axis, chunk, slots[k], lambda mine: reduce(k + 1, mine))
            return
        own = block_at({axis: lax.axis_index(axis) for axis in ("x", "z")})
        own[...] = (chunk[...] / replicas).astype(jnp.bfloat16)
        gather(0)

    reduce(0, part)


def kernel(replicas, a_hbm, b_hbm, out, a_ref, b_ref, for_x, for_z, ruler, in_sems, send_sems, recv_sems, *refs):
    work = units()
    parts, refs = refs[: len(work)], list(refs[len(work) :])
    slots = []
    for _, _, plan in work:
        slots.append([(refs.pop(0), refs.pop(0)) if kind == "coded" else refs.pop(0) for kind, _ in plan[0]])
    height, width = LEAF
    rows, tokens = for_x.shape
    extent = SIZE["z"] * width

    cuts = in_sems.shape[0] - 1
    load_a = pltpu.make_async_copy(a_hbm, a_ref, in_sems.at[cuts])
    load_a.start()
    loads_b = []
    for i in range(cuts):
        cut = pl.ds(i * (tokens // cuts), tokens // cuts)
        loads_b.append(pltpu.make_async_copy(b_hbm.at[cut], b_ref.at[cut], in_sems.at[i]))
        loads_b[-1].start()

    barrier = pltpu.get_barrier_semaphore()
    peers = 0
    for axis, n in SIZE.items():
        for delta in range(1, n):
            peer = wrapped(lax.axis_index(axis) + delta, n)
            pl.semaphore_signal(barrier, inc=1, device_id={axis: peer}, device_id_type=MESH)
            peers += 1

    group = 2 * height
    load_a.wait()
    for first in range(0, rows, 128):
        turned = a_ref[:, first : first + 128].T
        for row in range(first, first + 128, height):
            half, rest = divmod(row, rows // 2)
            x, rest = divmod(rest, rows // 2 // SIZE["x"])
            strip = rest // height
            piece = turned[row - first : row - first + height]
            for_x[pl.ds((x * STRIPS + strip) * group + half * height, height), :] = piece
            for_z[pl.ds((strip * SIZE["x"] + x) * group + half * height, height), :] = piece
    for load in loads_b:
        load.wait()

    def part_of(strip, side):
        for unit, part in zip(work, parts):
            if unit[:2] == (strip, side):
                return part

    def multiply_x(x):
        for side in range(SIDES):
            strips = X_STRIPS[side]
            if strips == 0:
                continue
            left = for_x[pl.ds(pl.multiple_of(x * (STRIPS * group), group), strips * group), :]
            for z in range(0, SIZE["z"], 2):
                column = side * extent + z * width
                total = jnp.dot(left, b_ref[:, column : column + 2 * width], preferred_element_type=jnp.float32)
                for strip in range(strips):
                    for half in range(2):
                        top = strip * group + half * height
                        for k in range(2):
                            part_of(strip, side)[x, half, z + k] = total[top : top + height, k * width : (k + 1) * width]

    def multiply_z(z):
        for side in range(SIDES):
            split = X_STRIPS[side]
            if split == STRIPS:
                continue
            left = for_z[split * SIZE["x"] * group :, :]
            column = pl.multiple_of(side * extent + z * width, width)
            total = jnp.dot(left, b_ref[:, pl.ds(column, width)], preferred_element_type=jnp.float32)
            for strip in range(split, STRIPS):
                for x in range(SIZE["x"]):
                    for half in range(2):
                        top = ((strip - split) * SIZE["x"] + x) * group + half * height
                        part_of(strip, side)[z, half, x] = total[top : top + height]

    me = {axis: lax.axis_index(axis) for axis in SIZE}
    flow = Flow(send_sems, recv_sems, ruler)
    multiply_z(wrapped(me["z"] + SIZE["z"] // 2, SIZE["z"]))
    multiply_x(wrapped(me["x"] + SIZE["x"] // 2, SIZE["x"]))
    pl.semaphore_wait(barrier, peers)
    for number, unit in enumerate(work):
        start_unit(flow, number, unit, parts[number], slots[number], out, replicas)
    for far in range(SIZE["z"] // 2 - 1, 0, -1):
        if far < SIZE["x"] // 2:
            multiply_x(wrapped(me["x"] + far, SIZE["x"]))
            multiply_x(wrapped(me["x"] - far, SIZE["x"]))
        multiply_z(wrapped(me["z"] + far, SIZE["z"]))
        multiply_z(wrapped(me["z"] - far, SIZE["z"]))
    multiply_x(me["x"])
    multiply_z(me["z"])
    flow.run()


def local(activations, cotangents):
    tokens, rows = activations.shape
    columns = cotangents.shape[1]
    work = units()
    scratch = [
        pltpu.VMEM((tokens, rows), jnp.bfloat16),
        pltpu.VMEM((tokens, columns), jnp.bfloat16),
        pltpu.VMEM((rows, tokens), jnp.bfloat16),
        pltpu.VMEM((rows, tokens), jnp.bfloat16),
        pltpu.VMEM((RULER, 8, LEAF[1]), jnp.bfloat16),
        pltpu.SemaphoreType.DMA((5,)),
    ]
    parts, slots, waits = [], [], 0
    for _, _, plan in work:
        order = order_of(plan)
        parts.append(pltpu.VMEM(tuple(SIZE[axis] for axis in order) + LEAF, jnp.float32))
        for k, (kind, axis) in enumerate(plan[0]):
            chunk = tuple(SIZE[other] for other in order[k + 1 :]) + LEAF
            if kind == "coded":
                slots += [pltpu.VMEM((slots_of(kind, axis), coded_rows(chunk), LEAF[1]), jnp.bfloat16)] * 2
            else:
                slots.append(pltpu.VMEM((slots_of(kind, axis),) + chunk, jnp.float32))
        waits += sum(waits_of(kind, axis) for stages in plan for kind, axis in stages)
    scratch += [pltpu.SemaphoreType.DMA((len(work),)), pltpu.SemaphoreType.DMA((waits,))] + parts + slots
    replicas = math.prod(SIZE.values())
    shape = (SIZE["x"], STRIPS, LEAF[0], columns)
    out = pl.pallas_call(
        lambda *refs: kernel(replicas, *refs),
        out_shape=pltpu.VMEM(shape, jnp.bfloat16),
        in_specs=[pl.BlockSpec(memory_space=pl.ANY)] * 2,
        out_specs=pl.BlockSpec(memory_space=pltpu.VMEM),
        scratch_shapes=scratch,
        compiler_params=pltpu.CompilerParams(collective_id=0, has_side_effects=True),
        name="grad_sum",
    )(activations, cotangents)
    return out.reshape(rows // SIZE["pair"], columns)


def solution(mesh):
    split = Mesh(
        mesh.devices.reshape(mesh.shape["pair"], SIZE["x"], SIZE["z"], mesh.shape["ep"]),
        ("pair", "x", "z", "ep"),
    )
    placed = P(("pair", "x", "z"), "ep")
    return jax.shard_map(
        local, mesh=split, in_specs=(placed, placed), out_specs=P("pair", "ep"), check_vma=False
    )
```

```python
import heapq
import math

import jax
import jax.numpy as jnp
from jax import lax
from jax.experimental import pallas as pl
from jax.experimental.pallas import tpu as pltpu
from jax.sharding import Mesh
from jax.sharding import PartitionSpec as P

SIZE = {"pair": 2, "x": 4, "z": 8}
MESH = pl.DeviceIdType.MESH
LEAF = (16, 128)
STRIPS = 4
SIDES = 2
X_STRIPS = (3, 2)
X_FIRST = (("coded", "x"), ("direct", "pair"), ("direct", "z"))
Z_FIRST = (("coded", "z"), ("direct", "pair"), ("direct", "x"))
RING_X = (("direct", "z"), ("ring", "x"))
THEN_X = (("direct", "z"), ("direct", "x"))
THEN_Z = (("direct", "x"), ("direct", "z"))
GATHERS = (RING_X, THEN_Z, RING_X, RING_X, RING_X, RING_X, THEN_Z, THEN_X)
GROUP = 4
CODE_POWER, CODE_STEEP, CODE_LOW = 36, 120.0, 2.0**-3.45
RULER = 320
BYTES_PER_US = 46600.0
HOP_US, FURTHER_US, TASK_US = 2.65, 0.9, 0.15


def units():
    found = []
    for k in range(STRIPS):
        for side in range(SIDES):
            split = X_STRIPS[side]
            if k < split:
                found.append((k, side, (X_FIRST, GATHERS[len(found)])))
            if STRIPS - 1 - k >= split:
                found.append((STRIPS - 1 - k, side, (Z_FIRST, GATHERS[len(found)])))
    return found


def order_of(plan):
    return tuple(axis for _, axis in plan[0])


def wrapped(index, n):
    return lax.rem(index + n, n)


class Flow:
    def __init__(self, send_sems, recv_sems, ruler):
        self.send_sems, self.recv_sems, self.ruler = send_sems, recv_sems, ruler
        self.now, self.free, self.heap, self.waits = 0.0, {}, [], 0
        self.sent = {}

    def send(self, unit, copies, arriving, then):
        k = self.waits
        self.waits += 1
        latest = 0.0
        for distances, src, dst in copies:
            pltpu.make_async_remote_copy(
                src_ref=src,
                dst_ref=dst,
                send_sem=self.send_sems.at[unit],
                recv_sem=self.recv_sems.at[k],
                device_id={axis: wrapped(lax.axis_index(axis) + d, SIZE[axis]) for axis, d in distances.items()},
                device_id_type=MESH,
            ).start()
            size = math.prod(dst.shape) * jnp.dtype(dst.dtype).itemsize
            self.sent[unit] = self.sent.get(unit, 0) + size
            end = self.now
            for axis, d in distances.items():
                link = (axis, d > 0)
                self.free[link] = max(self.now, self.free.get(link, 0.0)) + abs(d) * size / BYTES_PER_US
                end = max(end, self.free[link])
            hops = sum(abs(d) for d in distances.values())
            latest = max(latest, end + HOP_US + FURTHER_US * (hops - 1))
        heapq.heappush(self.heap, (latest, k, arriving, then))

    def room(self, size):
        row = math.prod(self.ruler.shape[1:]) * jnp.dtype(self.ruler.dtype).itemsize
        assert size % row == 0 and size // row <= self.ruler.shape[0]
        return self.ruler.at[pl.ds(0, size // row)]

    def span(self, *refs):
        return self.room(sum(math.prod(ref.shape) * jnp.dtype(ref.dtype).itemsize for ref in refs))

    def run(self):
        while self.heap:
            at, k, arriving, then = heapq.heappop(self.heap)
            self.now = max(self.now, at) + TASK_US
            pltpu.make_async_copy(arriving, arriving, self.recv_sems.at[k]).wait()
            then()
        for unit, size in self.sent.items():
            total = self.room(size)
            pltpu.make_async_copy(total, total, self.send_sems.at[unit]).wait()


def add_into(dst, *sources):
    if len(dst.shape) > 3:
        for i in range(dst.shape[0]):
            add_into(dst.at[i], *(source.at[i] for source in sources))
    else:
        total = dst[...]
        for source in sources:
            total += source[...]
        dst[...] = total


def slots_of(kind, axis):
    n = SIZE[axis]
    return n - 1 if kind == "direct" or n == 2 else 2 * (n // 2)


def waits_of(kind, axis):
    return 1 if kind == "direct" else slots_of(kind, axis)


def deltas_of(n):
    return [d for far in range(1, n // 2 + 1) for d in ((far, -far) if 2 * far < n else (far,))]


def reduce_direct(flow, unit, axis, part, slots, done):
    n = SIZE[axis]
    me = lax.axis_index(axis)

    def arrived():
        add_into(part.at[me], *(slots.at[i] for i in range(n - 1)))
        done(part.at[me])

    copies = [({axis: d}, part.at[wrapped(me + d, n)], slots.at[i]) for i, d in enumerate(deltas_of(n))]
    flow.send(unit, copies, slots, arrived)


def gather_direct(flow, unit, axis, block_at, at, done):
    mine = block_at({**at, axis: lax.axis_index(axis)})
    deltas = deltas_of(SIZE[axis])
    flow.send(unit, [({axis: d}, mine, mine) for d in deltas], flow.span(*[mine] * len(deltas)), done)


def gather_ring(flow, unit, axis, block_at, at, done):
    n = SIZE[axis]
    me = lax.axis_index(axis)
    steps = n // 2
    left = [2]

    def advance(sign, step):
        place = {**at, axis: wrapped(me - sign * step, n)}
        block = block_at(place, sign if step == steps - 1 else 0)

        def arrived():
            if step + 1 < steps:
                advance(sign, step + 1)
                return
            left[0] -= 1
            if left[0] == 0:
                done()

        flow.send(unit, [({axis: sign}, block, block)], block, arrived)

    advance(1, 0)
    advance(-1, 0)


def magnitudes(x):
    return jnp.max(jnp.abs(x), axis=0)


def encode(x, scale):
    y = jnp.abs(x) * (CODE_STEEP * CODE_LOW / jnp.maximum(scale, 1e-35)) + CODE_LOW
    y4 = y * y * (y * y)
    y8 = y4 * y4
    y16 = y8 * y8
    y = y16 * y16 * y4
    return jnp.where(x < 0, -y, y).astype(jnp.bfloat16)


def decode(code, scale):
    y = code.astype(jnp.float32)
    root = jnp.exp(jnp.log(jnp.abs(y)) * (1 / CODE_POWER) - math.log(CODE_LOW))
    x = (root - 1) * (scale * (1 / CODE_STEEP))
    return jnp.where(y < 0, -x, x)


def coded_rows(shape):
    return math.prod(shape[:-1]) + 8


def groups_of(chunk):
    if len(chunk.shape) == 3:
        return [chunk.at[pl.ds(i, GROUP)] for i in range(0, chunk.shape[0], GROUP)]
    return [group for i in range(chunk.shape[0]) for group in groups_of(chunk.at[i])]


def group_rows(k):
    rows = GROUP * LEAF[0]
    return pl.ds(8 + k * rows, rows)


def write_code(chunk, wire):
    shape = (GROUP * LEAF[0] // 8, 8, LEAF[1])
    groups = groups_of(chunk)
    scale = magnitudes(groups[0][...].reshape(shape))
    for group in groups[1:]:
        scale = jnp.maximum(scale, magnitudes(group[...].reshape(shape)))
    scale = scale.astype(jnp.bfloat16)
    wire[pl.ds(0, 8), :] = scale
    scale = scale.astype(jnp.float32)
    for k, group in enumerate(groups):
        wire[group_rows(k), :] = encode(group[...].reshape(shape), scale).reshape(-1, LEAF[1])


def add_code(chunk, wire):
    shape = (GROUP * LEAF[0] // 8, 8, LEAF[1])
    scale = wire[pl.ds(0, 8), :].astype(jnp.float32)
    for k, group in enumerate(groups_of(chunk)):
        value = decode(wire[group_rows(k), :].reshape(shape), scale)
        group[...] += value.reshape(group.shape)


def reduce_coded(flow, unit, axis, part, slots, done):
    wires_in, wires_out = slots
    n = SIZE[axis]
    me = lax.axis_index(axis)
    steps = n // 2
    middle = part.shape[1] // 2
    left = [2]

    def advance(sign, step):
        index = step if sign > 0 else steps + step
        chunk = part.at[wrapped(me + sign * (steps - step), n)]
        nearer = part.at[wrapped(me + sign * (steps - step - 1), n)]
        if step == 0:
            half = pl.ds(0 if sign > 0 else middle, middle)
            chunk, nearer = chunk.at[half], nearer.at[half]
        rows = pl.ds(0, coded_rows(chunk.shape))
        source, target = wires_out.at[index, rows], wires_in.at[index, rows]

        def arrived():
            add_code(nearer, target)
            if step + 1 < steps:
                advance(sign, step + 1)
                return
            left[0] -= 1
            if left[0] == 0:
                done(part.at[me])

        write_code(chunk, source)
        flow.send(unit, [({axis: sign}, source, target)], target, arrived)

    advance(1, 0)
    advance(-1, 0)


REDUCE = {"direct": reduce_direct, "coded": reduce_coded}
GATHER = {"ring": gather_ring, "direct": gather_direct}


def start_unit(flow, number, unit, part, slots, out, replicas):
    strip, side, (reduce_plan, gather_plan) = unit
    height, width = LEAF
    extent = SIZE["z"] * width

    def block_at(at, half=0):
        x = at.get("x", pl.ds(0, SIZE["x"]))
        cols = pl.ds(side * extent, extent)
        if "z" in at:
            cols = pl.ds(pl.multiple_of(side * extent + at["z"] * width, width), width)
        if half and "z" in at:
            x = pl.ds(0 if half > 0 else SIZE["x"] // 2, SIZE["x"] // 2)
        elif half:
            cols = pl.ds(side * extent + (0 if half > 0 else extent // 2), extent // 2)
        return out.at[x, strip, :, cols]

    def gather(k):
        if k < len(gather_plan):
            kind, axis = gather_plan[k]
            rest = {other: lax.axis_index(other) for _, other in gather_plan[k + 1 :]}
            GATHER[kind](flow, number, axis, block_at, rest, lambda: gather(k + 1))

    def reduce(k, chunk):
        if k < len(reduce_plan):
            kind, axis = reduce_plan[k]
            REDUCE[kind](flow, number, axis, chunk, slots[k], lambda mine: reduce(k + 1, mine))
            return
        own = block_at({axis: lax.axis_index(axis) for axis in ("x", "z")})
        own[...] = (chunk[...] / replicas).astype(jnp.bfloat16)
        gather(0)

    reduce(0, part)


def kernel(replicas, a_hbm, b_hbm, out, a_ref, b_ref, for_x, for_z, ruler, in_sems, send_sems, recv_sems, *refs):
    work = units()
    parts, refs = refs[: len(work)], list(refs[len(work) :])
    slots = []
    for _, _, plan in work:
        slots.append([(refs.pop(0), refs.pop(0)) if kind == "coded" else refs.pop(0) for kind, _ in plan[0]])
    height, width = LEAF
    rows, tokens = for_x.shape
    extent = SIZE["z"] * width

    cuts = in_sems.shape[0] - 1
    load_a = pltpu.make_async_copy(a_hbm, a_ref, in_sems.at[cuts])
    load_a.start()
    loads_b = []
    for i in range(cuts):
        cut = pl.ds(i * (tokens // cuts), tokens // cuts)
        loads_b.append(pltpu.make_async_copy(b_hbm.at[cut], b_ref.at[cut], in_sems.at[i]))
        loads_b[-1].start()

    barrier = pltpu.get_barrier_semaphore()
    peers = 0
    for axis, n in SIZE.items():
        for delta in range(1, n):
            peer = wrapped(lax.axis_index(axis) + delta, n)
            pl.semaphore_signal(barrier, inc=1, device_id={axis: peer}, device_id_type=MESH)
            peers += 1

    group = 2 * height
    load_a.wait()
    for first in range(0, rows, 128):
        turned = a_ref[:, first : first + 128].T
        for row in range(first, first + 128, height):
            half, rest = divmod(row, rows // 2)
            x, rest = divmod(rest, rows // 2 // SIZE["x"])
            strip = rest // height
            piece = turned[row - first : row - first + height]
            for_x[pl.ds((x * STRIPS + strip) * group + half * height, height), :] = piece
            for_z[pl.ds((strip * SIZE["x"] + x) * group + half * height, height), :] = piece
    for load in loads_b:
        load.wait()

    def part_of(strip, side):
        for unit, part in zip(work, parts):
            if unit[:2] == (strip, side):
                return part

    def multiply_x(x):
        for side in range(SIDES):
            strips = X_STRIPS[side]
            if strips == 0:
                continue
            left = for_x[pl.ds(pl.multiple_of(x * (STRIPS * group), group), strips * group), :]
            for z in range(0, SIZE["z"], 2):
                column = side * extent + z * width
                total = jnp.dot(left, b_ref[:, column : column + 2 * width], preferred_element_type=jnp.float32)
                for strip in range(strips):
                    for half in range(2):
                        top = strip * group + half * height
                        for k in range(2):
                            part_of(strip, side)[x, half, z + k] = total[top : top + height, k * width : (k + 1) * width]

    def multiply_z(z):
        for side in range(SIDES):
            split = X_STRIPS[side]
            if split == STRIPS:
                continue
            left = for_z[split * SIZE["x"] * group :, :]
            column = pl.multiple_of(side * extent + z * width, width)
            total = jnp.dot(left, b_ref[:, pl.ds(column, width)], preferred_element_type=jnp.float32)
            for strip in range(split, STRIPS):
                for x in range(SIZE["x"]):
                    for half in range(2):
                        top = ((strip - split) * SIZE["x"] + x) * group + half * height
                        part_of(strip, side)[z, half, x] = total[top : top + height]

    me = {axis: lax.axis_index(axis) for axis in SIZE}
    flow = Flow(send_sems, recv_sems, ruler)
    multiply_z(wrapped(me["z"] + SIZE["z"] // 2, SIZE["z"]))
    multiply_x(wrapped(me["x"] + SIZE["x"] // 2, SIZE["x"]))
    pl.semaphore_wait(barrier, peers)
    for number, unit in enumerate(work):
        start_unit(flow, number, unit, parts[number], slots[number], out, replicas)
    for far in range(SIZE["z"] // 2 - 1, 0, -1):
        if far < SIZE["x"] // 2:
            multiply_x(wrapped(me["x"] + far, SIZE["x"]))
            multiply_x(wrapped(me["x"] - far, SIZE["x"]))
        multiply_z(wrapped(me["z"] + far, SIZE["z"]))
        multiply_z(wrapped(me["z"] - far, SIZE["z"]))
    multiply_x(me["x"])
    multiply_z(me["z"])
    flow.run()


def local(activations, cotangents):
    tokens, rows = activations.shape
    columns = cotangents.shape[1]
    work = units()
    scratch = [
        pltpu.VMEM((tokens, rows), jnp.bfloat16),
        pltpu.VMEM((tokens, columns), jnp.bfloat16),
        pltpu.VMEM((rows, tokens), jnp.bfloat16),
        pltpu.VMEM((rows, tokens), jnp.bfloat16),
        pltpu.VMEM((RULER, 8, LEAF[1]), jnp.bfloat16),
        pltpu.SemaphoreType.DMA((5,)),
    ]
    parts, slots, waits = [], [], 0
    for _, _, plan in work:
        order = order_of(plan)
        parts.append(pltpu.VMEM(tuple(SIZE[axis] for axis in order) + LEAF, jnp.float32))
        for k, (kind, axis) in enumerate(plan[0]):
            chunk = tuple(SIZE[other] for other in order[k + 1 :]) + LEAF
            if kind == "coded":
                slots += [pltpu.VMEM((slots_of(kind, axis), coded_rows(chunk), LEAF[1]), jnp.bfloat16)] * 2
            else:
                slots.append(pltpu.VMEM((slots_of(kind, axis),) + chunk, jnp.float32))
        waits += sum(waits_of(kind, axis) for stages in plan for kind, axis in stages)
    scratch += [pltpu.SemaphoreType.DMA((len(work),)), pltpu.SemaphoreType.DMA((waits,))] + parts + slots
    replicas = math.prod(SIZE.values())
    shape = (SIZE["x"], STRIPS, LEAF[0], columns)
    out = pl.pallas_call(
        lambda *refs: kernel(replicas, *refs),
        out_shape=pltpu.VMEM(shape, jnp.bfloat16),
        in_specs=[pl.BlockSpec(memory_space=pl.ANY)] * 2,
        out_specs=pl.BlockSpec(memory_space=pltpu.VMEM),
        scratch_shapes=scratch,
        compiler_params=pltpu.CompilerParams(collective_id=0, has_side_effects=True),
        name="grad_sum",
    )(activations, cotangents)
    return out.reshape(rows // SIZE["pair"], columns)


def solution(mesh):
    split = Mesh(
        mesh.devices.reshape(mesh.shape["pair"], SIZE["x"], SIZE["z"], mesh.shape["ep"]),
        ("pair", "x", "z", "ep"),
    )
    placed = P(("pair", "x", "z"), "ep")
    return jax.shard_map(
        local, mesh=split, in_specs=(placed, placed), out_specs=P("pair", "ep"), check_vma=False
    )
```

```python
import heapq
import math

import jax
import jax.numpy as jnp
from jax import lax
from jax.experimental import pallas as pl
from jax.experimental.pallas import tpu as pltpu
from jax.sharding import Mesh
from jax.sharding import PartitionSpec as P

SIZE = {"pair": 2, "x": 4, "z": 8}
MESH = pl.DeviceIdType.MESH
LEAF = (16, 128)
STRIPS = 4
SIDES = 2
X_STRIPS = (3, 2)
X_FIRST = (("coded", "x"), ("direct", "pair"), ("direct", "z"))
Z_FIRST = (("coded", "z"), ("direct", "pair"), ("direct", "x"))
RING_X = (("direct", "z"), ("ring", "x"))
THEN_X = (("direct", "z"), ("direct", "x"))
THEN_Z = (("direct", "x"), ("direct", "z"))
GATHERS = (RING_X, THEN_Z, RING_X, RING_X, RING_X, RING_X, THEN_Z, THEN_X)
GROUP = 4
CODE_POWER, CODE_STEEP, CODE_LOW = 36, 120.0, 2.0**-3.45
RULER = 320
BYTES_PER_US = 46600.0
HOP_US, FURTHER_US, TASK_US = 3.0, 0.9, 0.15


def units():
    found = []
    for k in range(STRIPS):
        for side in range(SIDES):
            split = X_STRIPS[side]
            if k < split:
                found.append((k, side, (X_FIRST, GATHERS[len(found)])))
            if STRIPS - 1 - k >= split:
                found.append((STRIPS - 1 - k, side, (Z_FIRST, GATHERS[len(found)])))
    return found


def order_of(plan):
    return tuple(axis for _, axis in plan[0])


def wrapped(index, n):
    return lax.rem(index + n, n)


class Flow:
    def __init__(self, send_sems, recv_sems, ruler):
        self.send_sems, self.recv_sems, self.ruler = send_sems, recv_sems, ruler
        self.now, self.free, self.heap, self.waits = 0.0, {}, [], 0
        self.sent = {}

    def send(self, unit, copies, arriving, then):
        k = self.waits
        self.waits += 1
        latest = 0.0
        for distances, src, dst in copies:
            pltpu.make_async_remote_copy(
                src_ref=src,
                dst_ref=dst,
                send_sem=self.send_sems.at[unit],
                recv_sem=self.recv_sems.at[k],
                device_id={axis: wrapped(lax.axis_index(axis) + d, SIZE[axis]) for axis, d in distances.items()},
                device_id_type=MESH,
            ).start()
            size = math.prod(dst.shape) * jnp.dtype(dst.dtype).itemsize
            self.sent[unit] = self.sent.get(unit, 0) + size
            end = self.now
            for axis, d in distances.items():
                link = (axis, d > 0)
                self.free[link] = max(self.now, self.free.get(link, 0.0)) + abs(d) * size / BYTES_PER_US
                end = max(end, self.free[link])
            hops = sum(abs(d) for d in distances.values())
            latest = max(latest, end + HOP_US + FURTHER_US * (hops - 1))
        heapq.heappush(self.heap, (latest, k, arriving, then))

    def room(self, size):
        row = math.prod(self.ruler.shape[1:]) * jnp.dtype(self.ruler.dtype).itemsize
        assert size % row == 0 and size // row <= self.ruler.shape[0]
        return self.ruler.at[pl.ds(0, size // row)]

    def span(self, *refs):
        return self.room(sum(math.prod(ref.shape) * jnp.dtype(ref.dtype).itemsize for ref in refs))

    def run(self):
        while self.heap:
            at, k, arriving, then = heapq.heappop(self.heap)
            self.now = max(self.now, at) + TASK_US
            pltpu.make_async_copy(arriving, arriving, self.recv_sems.at[k]).wait()
            then()
        for unit, size in self.sent.items():
            total = self.room(size)
            pltpu.make_async_copy(total, total, self.send_sems.at[unit]).wait()


def add_into(dst, *sources):
    if len(dst.shape) > 3:
        for i in range(dst.shape[0]):
            add_into(dst.at[i], *(source.at[i] for source in sources))
    else:
        total = dst[...]
        for source in sources:
            total += source[...]
        dst[...] = total


def slots_of(kind, axis):
    n = SIZE[axis]
    return n - 1 if kind == "direct" or n == 2 else 2 * (n // 2)


def waits_of(kind, axis):
    return 1 if kind == "direct" else slots_of(kind, axis)


def deltas_of(n):
    return [d for far in range(n // 2, 0, -1) for d in ((far, -far) if 2 * far < n else (far,))]


def reduce_direct(flow, unit, axis, part, slots, done):
    n = SIZE[axis]
    me = lax.axis_index(axis)

    def arrived():
        add_into(part.at[me], *(slots.at[i] for i in range(n - 1)))
        done(part.at[me])

    copies = [({axis: d}, part.at[wrapped(me + d, n)], slots.at[i]) for i, d in enumerate(deltas_of(n))]
    flow.send(unit, copies, slots, arrived)


def gather_direct(flow, unit, axis, block_at, at, done):
    mine = block_at({**at, axis: lax.axis_index(axis)})
    deltas = deltas_of(SIZE[axis])
    flow.send(unit, [({axis: d}, mine, mine) for d in deltas], flow.span(*[mine] * len(deltas)), done)


def gather_ring(flow, unit, axis, block_at, at, done):
    n = SIZE[axis]
    me = lax.axis_index(axis)
    steps = n // 2
    left = [2]

    def advance(sign, step):
        place = {**at, axis: wrapped(me - sign * step, n)}
        block = block_at(place, sign if step == steps - 1 else 0)

        def arrived():
            if step + 1 < steps:
                advance(sign, step + 1)
                return
            left[0] -= 1
            if left[0] == 0:
                done()

        flow.send(unit, [({axis: sign}, block, block)], block, arrived)

    advance(1, 0)
    advance(-1, 0)


def magnitudes(x):
    return jnp.max(jnp.abs(x), axis=0)


def encode(x, scale):
    y = jnp.abs(x) * (CODE_STEEP * CODE_LOW / jnp.maximum(scale, 1e-35)) + CODE_LOW
    y4 = y * y * (y * y)
    y8 = y4 * y4
    y16 = y8 * y8
    y = y16 * y16 * y4
    return jnp.where(x < 0, -y, y).astype(jnp.bfloat16)


def decode(code, scale):
    y = code.astype(jnp.float32)
    root = jnp.exp(jnp.log(jnp.abs(y)) * (1 / CODE_POWER) - math.log(CODE_LOW))
    x = (root - 1) * (scale * (1 / CODE_STEEP))
    return jnp.where(y < 0, -x, x)


def coded_rows(shape):
    return math.prod(shape[:-1]) + 8


def groups_of(chunk):
    if len(chunk.shape) == 3:
        return [chunk.at[pl.ds(i, GROUP)] for i in range(0, chunk.shape[0], GROUP)]
    return [group for i in range(chunk.shape[0]) for group in groups_of(chunk.at[i])]


def group_rows(k):
    rows = GROUP * LEAF[0]
    return pl.ds(8 + k * rows, rows)


def write_code(chunk, wire):
    shape = (GROUP * LEAF[0] // 8, 8, LEAF[1])
    groups = groups_of(chunk)
    scale = magnitudes(groups[0][...].reshape(shape))
    for group in groups[1:]:
        scale = jnp.maximum(scale, magnitudes(group[...].reshape(shape)))
    scale = scale.astype(jnp.bfloat16)
    wire[pl.ds(0, 8), :] = scale
    scale = scale.astype(jnp.float32)
    for k, group in enumerate(groups):
        wire[group_rows(k), :] = encode(group[...].reshape(shape), scale).reshape(-1, LEAF[1])


def add_code(chunk, wire):
    shape = (GROUP * LEAF[0] // 8, 8, LEAF[1])
    scale = wire[pl.ds(0, 8), :].astype(jnp.float32)
    for k, group in enumerate(groups_of(chunk)):
        value = decode(wire[group_rows(k), :].reshape(shape), scale)
        group[...] += value.reshape(group.shape)


def reduce_coded(flow, unit, axis, part, slots, done):
    wires_in, wires_out = slots
    n = SIZE[axis]
    me = lax.axis_index(axis)
    steps = n // 2
    middle = part.shape[1] // 2
    left = [2]

    def advance(sign, step):
        index = step if sign > 0 else steps + step
        chunk = part.at[wrapped(me + sign * (steps - step), n)]
        nearer = part.at[wrapped(me + sign * (steps - step - 1), n)]
        if step == 0:
            half = pl.ds(0 if sign > 0 else middle, middle)
            chunk, nearer = chunk.at[half], nearer.at[half]
        rows = pl.ds(0, coded_rows(chunk.shape))
        source, target = wires_out.at[index, rows], wires_in.at[index, rows]

        def arrived():
            add_code(nearer, target)
            if step + 1 < steps:
                advance(sign, step + 1)
                return
            left[0] -= 1
            if left[0] == 0:
                done(part.at[me])

        write_code(chunk, source)
        flow.send(unit, [({axis: sign}, source, target)], target, arrived)

    advance(1, 0)
    advance(-1, 0)


REDUCE = {"direct": reduce_direct, "coded": reduce_coded}
GATHER = {"ring": gather_ring, "direct": gather_direct}


def start_unit(flow, number, unit, part, slots, out, replicas):
    strip, side, (reduce_plan, gather_plan) = unit
    height, width = LEAF
    extent = SIZE["z"] * width

    def block_at(at, half=0):
        x = at.get("x", pl.ds(0, SIZE["x"]))
        cols = pl.ds(side * extent, extent)
        if "z" in at:
            cols = pl.ds(pl.multiple_of(side * extent + at["z"] * width, width), width)
        if half and "z" in at:
            x = pl.ds(0 if half > 0 else SIZE["x"] // 2, SIZE["x"] // 2)
        elif half:
            cols = pl.ds(side * extent + (0 if half > 0 else extent // 2), extent // 2)
        return out.at[x, strip, :, cols]

    def gather(k):
        if k < len(gather_plan):
            kind, axis = gather_plan[k]
            rest = {other: lax.axis_index(other) for _, other in gather_plan[k + 1 :]}
            GATHER[kind](flow, number, axis, block_at, rest, lambda: gather(k + 1))

    def reduce(k, chunk):
        if k < len(reduce_plan):
            kind, axis = reduce_plan[k]
            REDUCE[kind](flow, number, axis, chunk, slots[k], lambda mine: reduce(k + 1, mine))
            return
        own = block_at({axis: lax.axis_index(axis) for axis in ("x", "z")})
        own[...] = (chunk[...] / replicas).astype(jnp.bfloat16)
        gather(0)

    reduce(0, part)


def kernel(replicas, a_hbm, b_hbm, out, a_ref, b_ref, for_x, for_z, ruler, in_sems, send_sems, recv_sems, *refs):
    work = units()
    parts, refs = refs[: len(work)], list(refs[len(work) :])
    slots = []
    for _, _, plan in work:
        slots.append([(refs.pop(0), refs.pop(0)) if kind == "coded" else refs.pop(0) for kind, _ in plan[0]])
    height, width = LEAF
    rows, tokens = for_x.shape
    extent = SIZE["z"] * width

    cuts = in_sems.shape[0] - 1
    load_a = pltpu.make_async_copy(a_hbm, a_ref, in_sems.at[cuts])
    load_a.start()
    loads_b = []
    for i in range(cuts):
        cut = pl.ds(i * (tokens // cuts), tokens // cuts)
        loads_b.append(pltpu.make_async_copy(b_hbm.at[cut], b_ref.at[cut], in_sems.at[i]))
        loads_b[-1].start()

    barrier = pltpu.get_barrier_semaphore()
    peers = 0
    for axis, n in SIZE.items():
        for delta in range(1, n):
            peer = wrapped(lax.axis_index(axis) + delta, n)
            pl.semaphore_signal(barrier, inc=1, device_id={axis: peer}, device_id_type=MESH)
            peers += 1

    group = 2 * height
    load_a.wait()
    for first in range(0, rows, 128):
        turned = a_ref[:, first : first + 128].T
        for row in range(first, first + 128, height):
            half, rest = divmod(row, rows // 2)
            x, rest = divmod(rest, rows // 2 // SIZE["x"])
            strip = rest // height
            piece = turned[row - first : row - first + height]
            for_x[pl.ds((x * STRIPS + strip) * group + half * height, height), :] = piece
            for_z[pl.ds((strip * SIZE["x"] + x) * group + half * height, height), :] = piece
    for load in loads_b:
        load.wait()

    def part_of(strip, side):
        for unit, part in zip(work, parts):
            if unit[:2] == (strip, side):
                return part

    def multiply_x(x):
        for side in range(SIDES):
            strips = X_STRIPS[side]
            if strips == 0:
                continue
            left = for_x[pl.ds(pl.multiple_of(x * (STRIPS * group), group), strips * group), :]
            for z in range(0, SIZE["z"], 2):
                column = side * extent + z * width
                total = jnp.dot(left, b_ref[:, column : column + 2 * width], preferred_element_type=jnp.float32)
                for strip in range(strips):
                    for half in range(2):
                        top = strip * group + half * height
                        for k in range(2):
                            part_of(strip, side)[x, half, z + k] = total[top : top + height, k * width : (k + 1) * width]

    def multiply_z(z):
        for side in range(SIDES):
            split = X_STRIPS[side]
            if split == STRIPS:
                continue
            left = for_z[split * SIZE["x"] * group :, :]
            column = pl.multiple_of(side * extent + z * width, width)
            total = jnp.dot(left, b_ref[:, pl.ds(column, width)], preferred_element_type=jnp.float32)
            for strip in range(split, STRIPS):
                for x in range(SIZE["x"]):
                    for half in range(2):
                        top = ((strip - split) * SIZE["x"] + x) * group + half * height
                        part_of(strip, side)[z, half, x] = total[top : top + height]

    me = {axis: lax.axis_index(axis) for axis in SIZE}
    flow = Flow(send_sems, recv_sems, ruler)
    multiply_z(wrapped(me["z"] + SIZE["z"] // 2, SIZE["z"]))
    multiply_x(wrapped(me["x"] + SIZE["x"] // 2, SIZE["x"]))
    pl.semaphore_wait(barrier, peers)
    for number, unit in enumerate(work):
        start_unit(flow, number, unit, parts[number], slots[number], out, replicas)
    for far in range(SIZE["z"] // 2 - 1, 0, -1):
        if far < SIZE["x"] // 2:
            multiply_x(wrapped(me["x"] + far, SIZE["x"]))
            multiply_x(wrapped(me["x"] - far, SIZE["x"]))
        multiply_z(wrapped(me["z"] + far, SIZE["z"]))
        multiply_z(wrapped(me["z"] - far, SIZE["z"]))
    multiply_x(me["x"])
    multiply_z(me["z"])
    flow.run()


def local(activations, cotangents):
    tokens, rows = activations.shape
    columns = cotangents.shape[1]
    work = units()
    scratch = [
        pltpu.VMEM((tokens, rows), jnp.bfloat16),
        pltpu.VMEM((tokens, columns), jnp.bfloat16),
        pltpu.VMEM((rows, tokens), jnp.bfloat16),
        pltpu.VMEM((rows, tokens), jnp.bfloat16),
        pltpu.VMEM((RULER, 8, LEAF[1]), jnp.bfloat16),
        pltpu.SemaphoreType.DMA((5,)),
    ]
    parts, slots, waits = [], [], 0
    for _, _, plan in work:
        order = order_of(plan)
        parts.append(pltpu.VMEM(tuple(SIZE[axis] for axis in order) + LEAF, jnp.float32))
        for k, (kind, axis) in enumerate(plan[0]):
            chunk = tuple(SIZE[other] for other in order[k + 1 :]) + LEAF
            if kind == "coded":
                slots += [pltpu.VMEM((slots_of(kind, axis), coded_rows(chunk), LEAF[1]), jnp.bfloat16)] * 2
            else:
                slots.append(pltpu.VMEM((slots_of(kind, axis),) + chunk, jnp.float32))
        waits += sum(waits_of(kind, axis) for stages in plan for kind, axis in stages)
    scratch += [pltpu.SemaphoreType.DMA((len(work),)), pltpu.SemaphoreType.DMA((waits,))] + parts + slots
    replicas = math.prod(SIZE.values())
    shape = (SIZE["x"], STRIPS, LEAF[0], columns)
    out = pl.pallas_call(
        lambda *refs: kernel(replicas, *refs),
        out_shape=pltpu.VMEM(shape, jnp.bfloat16),
        in_specs=[pl.BlockSpec(memory_space=pl.ANY)] * 2,
        out_specs=pl.BlockSpec(memory_space=pltpu.VMEM),
        scratch_shapes=scratch,
        compiler_params=pltpu.CompilerParams(collective_id=0, has_side_effects=True),
        name="grad_sum",
    )(activations, cotangents)
    return out.reshape(rows // SIZE["pair"], columns)


def solution(mesh):
    split = Mesh(
        mesh.devices.reshape(mesh.shape["pair"], SIZE["x"], SIZE["z"], mesh.shape["ep"]),
        ("pair", "x", "z", "ep"),
    )
    placed = P(("pair", "x", "z"), "ep")
    return jax.shard_map(
        local, mesh=split, in_specs=(placed, placed), out_specs=P("pair", "ep"), check_vma=False
    )
```

```python
import heapq
import math

import jax
import jax.numpy as jnp
from jax import lax
from jax.experimental import pallas as pl
from jax.experimental.pallas import tpu as pltpu
from jax.sharding import Mesh
from jax.sharding import PartitionSpec as P

SIZE = {"pair": 2, "x": 4, "z": 8}
MESH = pl.DeviceIdType.MESH
LEAF = (16, 128)
STRIPS = 4
SIDES = 2
X_STRIPS = (3, 2)
X_FIRST = (("coded", "x"), ("direct", "pair"), ("direct", "z"))
Z_FIRST = (("coded", "z"), ("direct", "pair"), ("direct", "x"))
RING_X = (("direct", "z"), ("ring", "x"))
THEN_X = (("direct", "z"), ("direct", "x"))
THEN_Z = (("direct", "x"), ("direct", "z"))
GATHERS = (RING_X, THEN_Z, RING_X, RING_X, RING_X, RING_X, THEN_Z, THEN_X)
GROUP = 4
CODE_POWER, CODE_STEEP, CODE_LOW = 36, 120.0, 2.0**-3.45
RULER = 320
BYTES_PER_US = 46600.0
HOP_US, FURTHER_US, TASK_US = 3.0, 0.9, 0.15


def units():
    found = []
    for k in range(STRIPS):
        for side in range(SIDES):
            split = X_STRIPS[side]
            if k < split:
                found.append((k, side, (X_FIRST, GATHERS[len(found)])))
            if STRIPS - 1 - k >= split:
                found.append((STRIPS - 1 - k, side, (Z_FIRST, GATHERS[len(found)])))
    return found


def order_of(plan):
    return tuple(axis for _, axis in plan[0])


def wrapped(index, n):
    return lax.rem(index + n, n)


class Flow:
    def __init__(self, send_sems, recv_sems, ruler):
        self.send_sems, self.recv_sems, self.ruler = send_sems, recv_sems, ruler
        self.now, self.free, self.heap, self.waits = 0.0, {}, [], 0
        self.sent = {}

    def send(self, unit, copies, arriving, then):
        k = self.waits
        self.waits += 1
        latest = 0.0
        for distances, src, dst in copies:
            pltpu.make_async_remote_copy(
                src_ref=src,
                dst_ref=dst,
                send_sem=self.send_sems.at[unit],
                recv_sem=self.recv_sems.at[k],
                device_id={axis: wrapped(lax.axis_index(axis) + d, SIZE[axis]) for axis, d in distances.items()},
                device_id_type=MESH,
            ).start()
            size = math.prod(dst.shape) * jnp.dtype(dst.dtype).itemsize
            self.sent[unit] = self.sent.get(unit, 0) + size
            end = self.now
            for axis, d in distances.items():
                link = (axis, d > 0)
                self.free[link] = max(self.now, self.free.get(link, 0.0)) + abs(d) * size / BYTES_PER_US
                end = max(end, self.free[link])
            hops = sum(abs(d) for d in distances.values())
            latest = max(latest, end + HOP_US + FURTHER_US * (hops - 1))
        heapq.heappush(self.heap, (latest, k, arriving, then))

    def room(self, size):
        row = math.prod(self.ruler.shape[1:]) * jnp.dtype(self.ruler.dtype).itemsize
        assert size % row == 0 and size // row <= self.ruler.shape[0]
        return self.ruler.at[pl.ds(0, size // row)]

    def span(self, *refs):
        return self.room(sum(math.prod(ref.shape) * jnp.dtype(ref.dtype).itemsize for ref in refs))

    def run(self):
        while self.heap:
            at, k, arriving, then = heapq.heappop(self.heap)
            self.now = max(self.now, at) + TASK_US
            pltpu.make_async_copy(arriving, arriving, self.recv_sems.at[k]).wait()
            then()
        for unit, size in self.sent.items():
            total = self.room(size)
            pltpu.make_async_copy(total, total, self.send_sems.at[unit]).wait()


def add_into(dst, *sources):
    if len(dst.shape) > 3:
        for i in range(dst.shape[0]):
            add_into(dst.at[i], *(source.at[i] for source in sources))
    else:
        total = dst[...]
        for source in sources:
            total += source[...]
        dst[...] = total


def slots_of(kind, axis):
    n = SIZE[axis]
    return n - 1 if kind == "direct" or n == 2 else 2 * (n // 2)


def waits_of(kind, axis):
    return 1 if kind == "direct" else slots_of(kind, axis)


def deltas_of(n):
    return [d for far in range(n // 2, 0, -1) for d in ((far, -far) if 2 * far < n else (far,))]


def reduce_direct(flow, unit, axis, part, slots, done):
    n = SIZE[axis]
    me = lax.axis_index(axis)

    def arrived():
        add_into(part.at[me], *(slots.at[i] for i in range(n - 1)))
        done(part.at[me])

    copies = [({axis: d}, part.at[wrapped(me + d, n)], slots.at[i]) for i, d in enumerate(deltas_of(n))]
    flow.send(unit, copies, slots, arrived)


def gather_direct(flow, unit, axis, block_at, at, done):
    mine = block_at({**at, axis: lax.axis_index(axis)})
    deltas = deltas_of(SIZE[axis])
    flow.send(unit, [({axis: d}, mine, mine) for d in deltas], flow.span(*[mine] * len(deltas)), done)


def gather_ring(flow, unit, axis, block_at, at, done):
    n = SIZE[axis]
    me = lax.axis_index(axis)
    steps = n // 2
    left = [2]

    def advance(sign, step):
        place = {**at, axis: wrapped(me - sign * step, n)}
        block = block_at(place, sign if step == steps - 1 else 0)

        def arrived():
            if step + 1 < steps:
                advance(sign, step + 1)
                return
            left[0] -= 1
            if left[0] == 0:
                done()

        flow.send(unit, [({axis: sign}, block, block)], block, arrived)

    advance(1, 0)
    advance(-1, 0)


def magnitudes(x):
    return jnp.max(jnp.abs(x), axis=0)


def encode(x, scale):
    y = jnp.abs(x) * (CODE_STEEP * CODE_LOW / jnp.maximum(scale, 1e-35)) + CODE_LOW
    y4 = y * y * (y * y)
    y8 = y4 * y4
    y16 = y8 * y8
    y = y16 * y16 * y4
    return jnp.where(x < 0, -y, y).astype(jnp.bfloat16)


def decode(code, scale):
    y = code.astype(jnp.float32)
    root = jnp.exp(jnp.log(jnp.abs(y)) * (1 / CODE_POWER) - math.log(CODE_LOW))
    x = (root - 1) * (scale * (1 / CODE_STEEP))
    return jnp.where(y < 0, -x, x)


def coded_rows(shape):
    return math.prod(shape[:-1]) + 8


def groups_of(chunk):
    if len(chunk.shape) == 3:
        return [chunk.at[pl.ds(i, GROUP)] for i in range(0, chunk.shape[0], GROUP)]
    return [group for i in range(chunk.shape[0]) for group in groups_of(chunk.at[i])]


def group_rows(k):
    rows = GROUP * LEAF[0]
    return pl.ds(8 + k * rows, rows)


def write_code(chunk, wire):
    shape = (GROUP * LEAF[0] // 8, 8, LEAF[1])
    groups = groups_of(chunk)
    scale = magnitudes(groups[0][...].reshape(shape))
    for group in groups[1:]:
        scale = jnp.maximum(scale, magnitudes(group[...].reshape(shape)))
    scale = scale.astype(jnp.bfloat16)
    wire[pl.ds(0, 8), :] = scale
    scale = scale.astype(jnp.float32)
    for k, group in enumerate(groups):
        wire[group_rows(k), :] = encode(group[...].reshape(shape), scale).reshape(-1, LEAF[1])


def add_code(chunk, wire):
    shape = (GROUP * LEAF[0] // 8, 8, LEAF[1])
    scale = wire[pl.ds(0, 8), :].astype(jnp.float32)
    for k, group in enumerate(groups_of(chunk)):
        value = decode(wire[group_rows(k), :].reshape(shape), scale)
        group[...] += value.reshape(group.shape)


def reduce_coded(flow, unit, axis, part, slots, done):
    wires_in, wires_out = slots
    n = SIZE[axis]
    me = lax.axis_index(axis)
    steps = n // 2
    middle = part.shape[1] // 2
    left = [2]

    def advance(sign, step):
        index = step if sign > 0 else steps + step
        chunk = part.at[wrapped(me + sign * (steps - step), n)]
        nearer = part.at[wrapped(me + sign * (steps - step - 1), n)]
        if step == 0:
            half = pl.ds(0 if sign > 0 else middle, middle)
            chunk, nearer = chunk.at[half], nearer.at[half]
        rows = pl.ds(0, coded_rows(chunk.shape))
        source, target = wires_out.at[index, rows], wires_in.at[index, rows]

        def arrived():
            add_code(nearer, target)
            if step + 1 < steps:
                advance(sign, step + 1)
                return
            left[0] -= 1
            if left[0] == 0:
                done(part.at[me])

        write_code(chunk, source)
        flow.send(unit, [({axis: sign}, source, target)], target, arrived)

    advance(1, 0)
    advance(-1, 0)


REDUCE = {"direct": reduce_direct, "coded": reduce_coded}
GATHER = {"ring": gather_ring, "direct": gather_direct}


def start_unit(flow, number, unit, part, slots, out, replicas):
    strip, side, (reduce_plan, gather_plan) = unit
    height, width = LEAF
    extent = SIZE["z"] * width

    def block_at(at, half=0):
        x = at.get("x", pl.ds(0, SIZE["x"]))
        cols = pl.ds(side * extent, extent)
        if "z" in at:
            cols = pl.ds(pl.multiple_of(side * extent + at["z"] * width, width), width)
        if half and "z" in at:
            x = pl.ds(0 if half > 0 else SIZE["x"] // 2, SIZE["x"] // 2)
        elif half:
            cols = pl.ds(side * extent + (0 if half > 0 else extent // 2), extent // 2)
        return out.at[x, strip, :, cols]

    def gather(k):
        if k < len(gather_plan):
            kind, axis = gather_plan[k]
            rest = {other: lax.axis_index(other) for _, other in gather_plan[k + 1 :]}
            GATHER[kind](flow, number, axis, block_at, rest, lambda: gather(k + 1))

    def reduce(k, chunk):
        if k < len(reduce_plan):
            kind, axis = reduce_plan[k]
            REDUCE[kind](flow, number, axis, chunk, slots[k], lambda mine: reduce(k + 1, mine))
            return
        own = block_at({axis: lax.axis_index(axis) for axis in ("x", "z")})
        own[...] = (chunk[...] / replicas).astype(jnp.bfloat16)
        gather(0)

    reduce(0, part)


def kernel(replicas, a_hbm, b_hbm, out, a_ref, b_ref, for_x, for_z, ruler, in_sems, send_sems, recv_sems, *refs):
    work = units()
    parts, refs = refs[: len(work)], list(refs[len(work) :])
    slots = []
    for _, _, plan in work:
        slots.append([(refs.pop(0), refs.pop(0)) if kind == "coded" else refs.pop(0) for kind, _ in plan[0]])
    height, width = LEAF
    rows, tokens = for_x.shape
    extent = SIZE["z"] * width

    cuts = in_sems.shape[0] - 1
    load_a = pltpu.make_async_copy(a_hbm, a_ref, in_sems.at[cuts])
    load_a.start()
    loads_b = []
    for i in range(cuts):
        cut = pl.ds(i * (tokens // cuts), tokens // cuts)
        loads_b.append(pltpu.make_async_copy(b_hbm.at[cut], b_ref.at[cut], in_sems.at[i]))
        loads_b[-1].start()

    barrier = pltpu.get_barrier_semaphore()
    peers = 0
    for axis, n in SIZE.items():
        for delta in range(1, n):
            peer = wrapped(lax.axis_index(axis) + delta, n)
            pl.semaphore_signal(barrier, inc=1, device_id={axis: peer}, device_id_type=MESH)
            peers += 1

    group = 2 * height
    load_a.wait()
    for first in range(0, rows, 128):
        turned = a_ref[:, first : first + 128].T
        for row in range(first, first + 128, height):
            half, rest = divmod(row, rows // 2)
            x, rest = divmod(rest, rows // 2 // SIZE["x"])
            strip = rest // height
            piece = turned[row - first : row - first + height]
            for_x[pl.ds((x * STRIPS + strip) * group + half * height, height), :] = piece
            for_z[pl.ds((strip * SIZE["x"] + x) * group + half * height, height), :] = piece
    for load in loads_b:
        load.wait()

    def part_of(strip, side):
        for unit, part in zip(work, parts):
            if unit[:2] == (strip, side):
                return part

    def multiply_x(x):
        for side in range(SIDES):
            strips = X_STRIPS[side]
            if strips == 0:
                continue
            left = for_x[pl.ds(pl.multiple_of(x * (STRIPS * group), group), strips * group), :]
            for z in range(0, SIZE["z"], 2):
                column = side * extent + z * width
                total = jnp.dot(left, b_ref[:, column : column + 2 * width], preferred_element_type=jnp.float32)
                for strip in range(strips):
                    for half in range(2):
                        top = strip * group + half * height
                        for k in range(2):
                            part_of(strip, side)[x, half, z + k] = total[top : top + height, k * width : (k + 1) * width]

    def multiply_z(z):
        for side in range(SIDES):
            split = X_STRIPS[side]
            if split == STRIPS:
                continue
            left = for_z[split * SIZE["x"] * group :, :]
            column = pl.multiple_of(side * extent + z * width, width)
            total = jnp.dot(left, b_ref[:, pl.ds(column, width)], preferred_element_type=jnp.float32)
            for strip in range(split, STRIPS):
                for x in range(SIZE["x"]):
                    for half in range(2):
                        top = ((strip - split) * SIZE["x"] + x) * group + half * height
                        part_of(strip, side)[z, half, x] = total[top : top + height]

    me = {axis: lax.axis_index(axis) for axis in SIZE}
    flow = Flow(send_sems, recv_sems, ruler)
    multiply_z(wrapped(me["z"] + SIZE["z"] // 2, SIZE["z"]))
    multiply_x(wrapped(me["x"] + SIZE["x"] // 2, SIZE["x"]))
    pl.semaphore_wait(barrier, peers)
    for number, unit in sorted(enumerate(work), key=lambda entry: entry[1][2][0] != Z_FIRST):
        start_unit(flow, number, unit, parts[number], slots[number], out, replicas)
    for far in range(SIZE["z"] // 2 - 1, 0, -1):
        if far < SIZE["x"] // 2:
            multiply_x(wrapped(me["x"] + far, SIZE["x"]))
            multiply_x(wrapped(me["x"] - far, SIZE["x"]))
        multiply_z(wrapped(me["z"] + far, SIZE["z"]))
        multiply_z(wrapped(me["z"] - far, SIZE["z"]))
    multiply_x(me["x"])
    multiply_z(me["z"])
    flow.run()


def local(activations, cotangents):
    tokens, rows = activations.shape
    columns = cotangents.shape[1]
    work = units()
    scratch = [
        pltpu.VMEM((tokens, rows), jnp.bfloat16),
        pltpu.VMEM((tokens, columns), jnp.bfloat16),
        pltpu.VMEM((rows, tokens), jnp.bfloat16),
        pltpu.VMEM((rows, tokens), jnp.bfloat16),
        pltpu.VMEM((RULER, 8, LEAF[1]), jnp.bfloat16),
        pltpu.SemaphoreType.DMA((5,)),
    ]
    parts, slots, waits = [], [], 0
    for _, _, plan in work:
        order = order_of(plan)
        parts.append(pltpu.VMEM(tuple(SIZE[axis] for axis in order) + LEAF, jnp.float32))
        for k, (kind, axis) in enumerate(plan[0]):
            chunk = tuple(SIZE[other] for other in order[k + 1 :]) + LEAF
            if kind == "coded":
                slots += [pltpu.VMEM((slots_of(kind, axis), coded_rows(chunk), LEAF[1]), jnp.bfloat16)] * 2
            else:
                slots.append(pltpu.VMEM((slots_of(kind, axis),) + chunk, jnp.float32))
        waits += sum(waits_of(kind, axis) for stages in plan for kind, axis in stages)
    scratch += [pltpu.SemaphoreType.DMA((len(work),)), pltpu.SemaphoreType.DMA((waits,))] + parts + slots
    replicas = math.prod(SIZE.values())
    shape = (SIZE["x"], STRIPS, LEAF[0], columns)
    out = pl.pallas_call(
        lambda *refs: kernel(replicas, *refs),
        out_shape=pltpu.VMEM(shape, jnp.bfloat16),
        in_specs=[pl.BlockSpec(memory_space=pl.ANY)] * 2,
        out_specs=pl.BlockSpec(memory_space=pltpu.VMEM),
        scratch_shapes=scratch,
        compiler_params=pltpu.CompilerParams(collective_id=0, has_side_effects=True),
        name="grad_sum",
    )(activations, cotangents)
    return out.reshape(rows // SIZE["pair"], columns)


def solution(mesh):
    split = Mesh(
        mesh.devices.reshape(mesh.shape["pair"], SIZE["x"], SIZE["z"], mesh.shape["ep"]),
        ("pair", "x", "z", "ep"),
    )
    placed = P(("pair", "x", "z"), "ep")
    return jax.shard_map(
        local, mesh=split, in_specs=(placed, placed), out_specs=P("pair", "ep"), check_vma=False
    )
```
